32 devices in a mesh: rows: 8 (over z, y), hosts: 4 (over x, core).
Axes of the slice: x: 2, y: 2, z: 4, core: 2. Of those that a mesh axis runs over, the one named last changes fastest.
Arguments:
- embeddings: float32 [32768, 768], P(('rows', 'hosts')), may hold values from -6 to 6
- root_centroids: float32 [512, 768], replicated, may hold values from -6 to 6
- member_ids: int32 [3, 32768], P(None, ('rows', 'hosts')), may hold values from 0 to 511
- split_order: int32 [3, 512], replicated, may hold values from 0 to 511, each once within a row
- seed_rows: int32 [3, 256, 2], replicated, may hold values from 0 to 32767
Outputs:
- centroids: float32 [512, 768], replicated
- spread: float32 [3, 512], replicated
- child_weight: float32 [3, 32768], P(None, ('rows', 'hosts'))
The draws below stay inside these ranges and needn't reach their ends.
Inputs may be any that keep to these rules, and one draw needn't show every extreme that they name: Each row of split_order names every cluster number once; its first 256 entries are the clusters split at that level.
All inputs are finite; a program needn't handle non-finite values.
Results may differ from the reference program's by a relative error of at most 0.0003.
Values sent between devices are 32-bit elements; how exact they have to be, the bound alone decides.
No kernel may reach another device: no remote copies, remote signals or barrier semaphores. Data moves between devices by JAX's collectives and lax.ppermute only.
A program may use at most 64 MiB of HBM per device.

```python
import jax
import jax.numpy as jnp
from jax import lax

E = 768
SPLITS = 256
LEVELS = 3
CLUSTERS = 512
TOTAL_ROWS = 32768


def place_ends(entries, stream_key, least, top_value):
    extent = entries.shape
    place = [jax.random.randint(jax.random.fold_in(stream_key, axis), (), 0, extent[axis]) for axis in range(len(extent))]
    entries = entries.at[tuple(place)].set(least)
    longest = extent.index(max(extent))
    place[longest] = (place[longest] + 1) % extent[longest]
    return entries.at[tuple(place)].set(top_value)


def levels(key, shape, split, least, high):
    def one(dim, blocks):
        steps = jax.random.uniform(jax.random.fold_in(jax.random.fold_in(key, 6), dim), (blocks,), jnp.float32, least / len(split), high / len(split))
        return jnp.repeat(jnp.exp(steps), shape[dim] // blocks).reshape((-1,) + (1,) * (len(shape) - dim - 1))

    gain = one(*split[0])
    for cut in split[1:]:
        gain = gain * one(*cut)
    return gain


def noise(stream_key, dims, scale, bound, cuts=(), dtype=jnp.bfloat16):
    loudness = levels(stream_key, dims, cuts, -0.22, 0.18) if cuts else 1.0
    result = jax.random.normal(stream_key, dims, jnp.float32) * scale * loudness
    return jnp.minimum(jnp.maximum(result, -bound), bound).astype(dtype)


def setup_inputs(seed: int = 0) -> dict:
    key_of = jax.random.split(jax.random.key(seed), 6)
    embeddings = noise(key_of[0], (TOTAL_ROWS, E), 1.0, 6.0, ((0, 32),), jnp.float32)
    root_centroids = noise(key_of[1], (CLUSTERS, E), 1.0, 6.0, (), jnp.float32)
    member_ids = place_ends(jax.random.randint(key_of[2], (LEVELS, TOTAL_ROWS), 0, CLUSTERS), jax.random.fold_in(key_of[2], 1), 0, CLUSTERS - 1).astype(jnp.int32)
    split_order = jax.vmap(lambda own: jax.random.permutation(own, CLUSTERS))(jax.random.split(key_of[3], LEVELS)).reshape((LEVELS, CLUSTERS)).astype(jnp.int32)
    seed_rows = place_ends(jax.random.randint(key_of[4], (LEVELS, SPLITS, 2), 0, TOTAL_ROWS), jax.random.fold_in(key_of[4], 1), 0, TOTAL_ROWS - 1).astype(jnp.int32)
    return dict(embeddings=embeddings, root_centroids=root_centroids, member_ids=member_ids, split_order=split_order, seed_rows=seed_rows)


def reference(embeddings, root_centroids, member_ids, split_order, seed_rows):
    high = lax.Precision.HIGHEST
    width = embeddings.shape[1]
    scale = 0.5 / jnp.sqrt(jnp.float32(width))
    squares = lax.optimization_barrier(jnp.sum(embeddings * embeddings, axis=1))
    current = root_centroids
    spreads = []
    weights_out = []
    for level in range(LEVELS):
        splits = split_order[level, :SPLITS]
        parent = jnp.take(current, splits, axis=0)
        picked = jnp.take(embeddings, seed_rows[level], axis=0)
        seeds = 0.5 * (parent[:, None, :] + picked)
        delta = seeds[:, 0, :] - seeds[:, 1, :]
        offset = lax.optimization_barrier(jnp.sum(seeds[:, 1, :] ** 2, axis=1)) - lax.optimization_barrier(jnp.sum(seeds[:, 0, :] ** 2, axis=1))
        chosen = (member_ids[level][:, None] == splits[None, :]).astype(jnp.float32)
        projected = jnp.dot(embeddings, delta.T, precision=high)
        gap = lax.optimization_barrier(jnp.sum(chosen * (2.0 * projected + offset[None, :]), axis=1))
        first = jax.nn.sigmoid(gap * scale)
        inside = lax.optimization_barrier(jnp.sum(chosen, axis=1))
        weights_out.append(first * inside)
        weights = jnp.stack([chosen * first[:, None], chosen * (1.0 - first)[:, None]], axis=2)
        weights = weights.reshape(weights.shape[0], 2 * SPLITS)
        sums = lax.dot_general(weights, embeddings, (((0,), (0,)), ((), ())), precision=high)
        counts = lax.optimization_barrier(jnp.sum(weights, axis=0))
        energy = jnp.dot(squares, weights, precision=high)
        seeds_flat = seeds.reshape(2 * SPLITS, width)
        current = (sums + seeds_flat) / (counts + 1.0)[:, None]
        error = energy - 2.0 * lax.optimization_barrier(jnp.sum(current * sums, axis=1)) + counts * lax.optimization_barrier(jnp.sum(current * current, axis=1))
        spreads.append(error / ((counts + 1.0) * width))
    return (current, jnp.stack(spreads), jnp.stack(weights_out))
```

```python
import jax
import jax.numpy as jnp
from jax import lax
from jax.sharding import PartitionSpec as P

AXES = ("rows", "hosts")


def stages_of(devices):
    bits = devices.bit_length() - 1
    if 1 << bits != devices:
        raise ValueError("device count")
    return [2] * (bits % 2) + [4] * (bits // 2)


class Comm:
    def __init__(self, devices):
        self.n = devices
        self.me = lax.axis_index(AXES)
        self.radices = stages_of(devices)
        self.strides = []
        step = 1
        for radix in self.radices:
            self.strides.append(step)
            step *= radix
        self.digits = [(self.me // s) % r for s, r in zip(self.strides, self.radices)]
        block = 0
        for digit, radix in zip(self.digits, self.radices):
            block = block * radix + digit
        self.block = block

    def send(self, x, mask):
        return lax.ppermute(x, AXES, [(i, i ^ mask) for i in range(self.n)])

    def reduce_scatter(self, x):
        x = x.reshape(tuple(self.radices) + x.shape[1:])
        for digit, radix, stride in zip(self.digits, self.radices, self.strides):
            got = [
                self.send(lax.dynamic_index_in_dim(x, digit ^ j, 0, False), j * stride)
                for j in range(1, radix)
            ]
            x = lax.dynamic_index_in_dim(x, digit, 0, False)
            for g in got:
                x = x + g
        return x

    def all_gather(self, x):
        shape = x.shape
        for radix, stride in zip(self.radices[::-1], self.strides[::-1]):
            x = jnp.stack([x] + [self.send(x, j * stride) for j in range(1, radix)])
        x = x.reshape((self.n,) + shape)
        return jnp.take(x, jnp.arange(self.n) ^ self.block, axis=0)

    def all_reduce(self, x):
        for radix, stride in zip(self.radices, self.strides):
            total = x
            for j in range(1, radix):
                total = total + self.send(x, j * stride)
            x = total
        return x


def parts_of(x):
    high = lax.reduce_precision(x, 8, 7)
    rest = x - high
    middle = lax.reduce_precision(rest, 8, 7)
    low = rest - middle
    return [p.astype(jnp.bfloat16) for p in (high, middle, low)]


def exact_dot(selector, parts):
    out = None
    for p in parts:
        t = lax.dot_general(
            selector, p, (((1,), (0,)), ((), ())), preferred_element_type=jnp.float32
        )
        out = t if out is None else out + t
    return out


def on_device(embeddings, root_centroids, member_ids, split_order, seed_rows):
    rows_dev, width = embeddings.shape
    levels, splits_count = seed_rows.shape[:2]
    comm = Comm(lax.axis_size(AXES))
    n = comm.n
    own = splits_count // n
    first_row = comm.me * rows_dev
    scale = 0.5 / jnp.sqrt(jnp.float32(width))
    squares = jnp.sum(embeddings * embeddings, axis=1)
    parts = parts_of(embeddings)
    splits = split_order[:, :splits_count]
    local = seed_rows - first_row
    row = lax.broadcasted_iota(jnp.int32, (splits_count, rows_dev), 1)
    high = lax.Precision.HIGH

    def blocks(x):
        return x.reshape((n, own) + x.shape[1:])

    def mine(x):
        return lax.dynamic_slice_in_dim(x, comm.block * own, own, 0)

    delta_loc, delta_own, delta, b_loc = [], [], [], []
    for l in range(levels):
        hot0 = (local[l, :, 0][:, None] == row).astype(jnp.float32)
        hot1 = (local[l, :, 1][:, None] == row).astype(jnp.float32)
        part = exact_dot((0.5 * (hot0 - hot1)).astype(jnp.bfloat16), parts)
        delta_loc.append(part)
        b_loc.append(0.25 * jnp.sum((hot0 - hot1) * squares[None, :], axis=1))
        got = comm.reduce_scatter(blocks(part))
        delta_own.append(got)
        delta.append(comm.all_gather(got).reshape(splits_count, width))
    b = comm.all_reduce(jnp.stack(b_loc))
    mean_loc = []
    for l in range(levels):
        hot0 = (local[l, :, 0][:, None] == row).astype(jnp.float32)
        hot1 = (local[l, :, 1][:, None] == row).astype(jnp.float32)
        mean_loc.append(exact_dot((0.5 * (hot0 + hot1)).astype(jnp.bfloat16), parts))

    project = [
        lax.dot_general(d, embeddings, (((1,), (1,)), ((), ())), precision=high) for d in delta
    ]
    ancestors = []
    rootdot = []
    for l in range(levels):
        chain = {}
        node = splits[l]
        for k in range(l - 1, -1, -1):
            chain[k] = node
            node = jnp.take(splits[k], node // 2)
        ancestors.append(chain)
        rootdot.append(jnp.sum(jnp.take(root_centroids, node, axis=0) * delta[l], axis=1))

    index, weight0, weight1 = [], [], []
    inverse = []
    weights_out = []
    spread_own = []
    centre_own = None
    is_root = (comm.me == 0).astype(jnp.float32)
    mid = 0.5 * (mean_loc[0] + is_root * jnp.take(root_centroids, splits[0], axis=0))
    dots = rootdot[0]
    for l in range(levels):
        offset = 0.5 * (dots + b[l])
        chosen = (splits[l][:, None] == member_ids[l][None, :]).astype(jnp.float32)
        gap = 2.0 * jnp.sum(chosen * (project[l] - offset[:, None]), axis=0)
        inside = jnp.sum(chosen, axis=0)
        first = jax.nn.sigmoid(gap * scale)
        weights_out.append(first * inside)
        split_id = lax.broadcasted_iota(jnp.int32, (splits_count, rows_dev), 0)
        index.append(
            jnp.sum(jnp.where(chosen > 0, split_id, 0), axis=0)
            - jnp.where(inside > 0, 0, 1)
        )
        weight0.append(first)
        weight1.append(1.0 - first)
        w0 = chosen * first[None, :]
        w1 = chosen * (1.0 - first)[None, :]
        small = [
            jnp.sum(w0, axis=1),
            jnp.sum(w1, axis=1),
            jnp.sum(w0 * squares[None, :], axis=1),
            jnp.sum(w1 * squares[None, :], axis=1),
        ]
        coefs = []
        if l + 1 < levels:
            coef = jnp.ones((splits_count,), jnp.float32)
            dot = jnp.zeros((splits_count,), jnp.float32)
            for k in range(l, -1, -1):
                child = ancestors[l + 1][k]
                if k < l:
                    coef = coef * jnp.take(inverse[k], child)
                half = child % 2
                hit = index[k][None, :] == (child // 2)[:, None]
                w = jnp.where(
                    hit,
                    jnp.where(half[:, None] == 0, weight0[k][None, :], weight1[k][None, :]),
                    0.0,
                )
                seed = jnp.take(local[k].reshape(-1), child)
                w = w + 0.5 * (seed[:, None] == row)
                dot = dot + coef * jnp.sum(w * project[l + 1], axis=1)
                coef = 0.5 * coef
            small.append(dot)
        small = comm.all_reduce(jnp.stack(small))
        count = jnp.stack([small[0], small[1]], axis=1)
        energy = jnp.stack([small[2], small[3]], axis=1)
        inverse.append((1.0 / (count + 1.0)).reshape(-1))
        if l + 1 < levels:
            dots = (small[4] + coef * rootdot[l + 1]) * jnp.take(inverse[l], splits[l + 1])
        sums = [
            lax.dot_general(w, embeddings, (((1,), (0,)), ((), ())), precision=high)
            for w in (w0, w1)
        ]
        payload = jnp.stack([blocks(sums[0]), blocks(sums[1]), blocks(mid)], axis=1)
        got = comm.reduce_scatter(payload)
        s_own = jnp.stack([got[0], got[1]], axis=1)
        half = 0.5 * delta_own[l]
        seed_own = jnp.stack([got[2] + half, got[2] - half], axis=1)
        c_own, e_own = mine(count), mine(energy)
        centre_own = (s_own + seed_own) / (c_own + 1.0)[..., None]
        error = (
            e_own
            - 2.0 * jnp.sum(centre_own * s_own, axis=2)
            + c_own * jnp.sum(centre_own * centre_own, axis=2)
        )
        spread_own.append(error / ((c_own + 1.0) * width))
        if l + 1 < levels:
            half = 0.5 * delta_loc[l]
            total = jnp.stack([sums[0] + mid + half, sums[1] + mid - half], axis=1)
            total = total.reshape(2 * splits_count, width) * inverse[l][:, None]
            mid = 0.5 * (jnp.take(total, splits[l + 1], axis=0) + mean_loc[l + 1])
    centre = comm.all_gather(centre_own).reshape(2 * splits_count, width)
    spread = comm.all_gather(jnp.stack(spread_own))
    spread = spread.transpose(1, 0, 2, 3).reshape(levels, 2 * splits_count)
    return (centre, spread, jnp.stack(weights_out))


def solution(mesh):
    in_specs = (P(AXES, None), P(), P(None, AXES), P(), P())
    out_specs = (P(), P(), P(None, AXES))
    return jax.shard_map(
        on_device, mesh=mesh, in_specs=in_specs, out_specs=out_specs, check_vma=False
    )
```

```python
import functools

import jax
import jax.numpy as jnp
from jax import lax
from jax.experimental import pallas as pl
from jax.experimental.pallas import tpu as pltpu
from jax.sharding import PartitionSpec as P

AXES = ("rows", "hosts")
LANES = 128
F32 = jnp.float32
BF16 = jnp.bfloat16


class Comm:
    def __init__(self, devices, most_blocks):
        self.n = devices
        self.me = lax.axis_index(AXES)
        bits = devices.bit_length() - 1
        assert 1 << bits == devices
        radices = [2] * (bits % 2) + [4] * (bits // 2)
        self.stages, self.extra = [], []
        self.blocks, stride, self.block = 1, 1, 0
        for radix in radices:
            if self.blocks * radix <= most_blocks:
                self.stages.append((radix, stride))
                self.block = self.block * radix + (self.me // stride) % radix
                self.blocks *= radix
            else:
                self.extra.append((radix, stride))
            stride *= radix
        self.lead = self.stages[0][0]

    def send(self, x, mask):
        return lax.ppermute(x, AXES, [(i, i ^ mask) for i in range(self.n)])

    def reduce_scatter(self, pieces):
        for step, (radix, stride) in enumerate(self.stages):
            if step:
                x = x.reshape((radix, x.shape[0] // radix) + x.shape[1:])
                pieces = [x[j] for j in range(radix)]
            got = [self.send(pieces[j], j * stride) for j in range(1, radix)]
            x = functools.reduce(jnp.add, got, pieces[0])
        x = x[0]
        for radix, stride in self.extra:
            while radix > 1:
                x = x + self.send(x, stride)
                stride, radix = stride * 2, radix // 2
        return x

    def all_gather(self, x):
        x = x[None]
        for radix, stride in self.stages[::-1]:
            pieces = [x] + [self.send(x, j * stride) for j in range(1, radix)]
            if (radix, stride) != self.stages[0]:
                x = jnp.concatenate(pieces)
        return pieces

    def share(self, x):
        return lax.all_to_all(x, AXES, 0, 0, tiled=True)


def dot(a, b):
    return lax.dot_general(a, b, (((1,), (0,)), ((), ())), preferred_element_type=F32)


def dot_t(a, b):
    return lax.dot_general(a, b, (((1,), (1,)), ((), ())), preferred_element_type=F32)


def split2(x):
    high = x.astype(BF16)
    return high, (x - high.astype(F32)).astype(BF16)


def iota(shape, axis):
    return lax.broadcasted_iota(jnp.int32, shape, axis)


def lane_sum(x):
    return jnp.sum(x, axis=1, keepdims=True)


def pack(columns):
    rows = columns[0].shape[0]
    lane = iota((rows, LANES), 1)
    out = jnp.zeros((rows, LANES), F32)
    for q, c in enumerate(columns):
        out = jnp.where(lane == q, c, out)
    return out


def to_blocks(scratch, outs, block, own, per):
    for j, out in enumerate(outs):
        for t in range(per):
            at = (block ^ (j * per + t)) * own
            out[t] = scratch[pl.ds(pl.multiple_of(at, 8), own), :]


def from_blocks(pieces, scratch, block, own, per):
    for j, piece in enumerate(pieces):
        for t in range(per):
            at = (block ^ (j * per + t)) * own
            scratch[pl.ds(pl.multiple_of(at, 8), own), :] = piece[t]


def pick_kernel(place, seeds, emb, *refs, levels, lead, per, own):
    outs = refs[:lead]
    high, low, delta, mean, scratch = refs[lead:]
    rows, width = emb.shape
    splits = seeds.shape[1]
    e = emb[...]
    a = e.astype(BF16)
    rest = e - a.astype(F32)
    b = rest.astype(BF16)
    c = (rest - b.astype(F32)).astype(BF16)
    high[...] = a
    low[...] = b
    row = iota((splits, rows), 1) + place[1]
    bs = []
    for l in range(levels):
        hot0 = jnp.where(seeds[l, :, 0:1] == row, 0.5, 0.0)
        hot1 = jnp.where(seeds[l, :, 1:2] == row, 0.5, 0.0)
        d = (hot0 - hot1).astype(BF16)
        m = (hot0 + hot1).astype(BF16)
        dv = dot(d, a) + (dot(d, b) + dot(d, c))
        mv = dot(m, a) + (dot(m, b) + dot(m, c))
        delta[l] = dv
        mean[l] = mv
        scratch[:, l * width : (l + 1) * width] = dv
        bs.append(lane_sum(dv * mv))
    scratch[:, levels * width :] = pack(bs)
    to_blocks(scratch, outs, place[0], own, per)


def level_step(l, levels, offset, proj, cols, member, sq, rows_in, lookups, scale):
    splits, rows = proj.shape[1:]
    chosen = cols[:, l : l + 1] == member[l : l + 1, :]
    part = jnp.where(chosen, proj[l] - offset, 0.0)
    gap = 2.0 * jnp.sum(part, axis=0, keepdims=True)
    inside = jnp.sum(jnp.where(chosen, 1.0, 0.0), axis=0, keepdims=True)
    first = jax.nn.sigmoid(gap * scale)
    number = iota((splits, rows), 0).astype(F32)
    index = jnp.sum(jnp.where(chosen, number + 1.0, 0.0), axis=0, keepdims=True) - 1.0
    w0 = jnp.where(chosen, first, 0.0)
    w1 = jnp.where(chosen, 1.0 - first, 0.0)
    columns = [lane_sum(w0), lane_sum(w1), lane_sum(w0 * sq), lane_sum(w1 * sq)]
    rows_out = rows_in + [(index, first)]
    if l + 1 < levels:
        row = iota((splits, rows), 1)
        coef = jnp.ones((splits, 1), F32)
        total = jnp.zeros((splits, 1), F32)
        for k in range(l, -1, -1):
            half, odd, seed = ancestor(cols, levels, l + 1, k)
            if k < l:
                coef = coef * lookups[k](half, odd)
            at, f = rows_out[k]
            w = jnp.where(at == half.astype(F32), jnp.where(odd > 0, 1.0 - f, f), 0.0)
            w = w + jnp.where(row == seed, 0.5, 0.0)
            total = total + coef * lane_sum(w * proj[l + 1])
            coef = 0.5 * coef
        columns += [total, coef]
    return first * inside, rows_out, columns


def ancestor(cols, levels, l, k):
    at = 2 * levels + 3 * (l * (l - 1) // 2 + k)
    return cols[:, at : at + 1], cols[:, at + 1 : at + 2], cols[:, at + 2 : at + 3]


def emit(columns, small, shared, n):
    packed = pack(columns)
    small[...] = packed
    across = jnp.transpose(packed)[:8, :]
    for i in range(n):
        shared[i] = across


def project_kernel(place, *refs, levels, lead, per, own, n, scale):
    pieces = refs[:lead]
    high, low, emb, root, cols, member = refs[lead : lead + 6]
    proj, stat, small, shared, state, out, scratch = refs[lead + 6 :]
    rows, width = emb.shape
    splits = proj.shape[1]
    from_blocks(pieces, scratch, place[0], own, per)
    e = emb[...]
    q = e * e
    ones = jnp.ones((8, width), BF16)
    qa = q.astype(BF16)
    rest = q - qa.astype(F32)
    qb = rest.astype(BF16)
    qc = (rest - qb.astype(F32)).astype(BF16)
    sq = (dot_t(ones, qa) + (dot_t(ones, qb) + dot_t(ones, qc)))[0:1, :]
    a, b = high[...], low[...]
    ra, rb = split2(root[...])
    lane = iota((splits, root.shape[0]), 1)
    stats = [scratch[:, levels * width + l : levels * width + l + 1] for l in range(levels)]
    for l in range(levels):
        da, db = split2(scratch[:, l * width : (l + 1) * width])
        proj[l] = dot_t(da, a) + (dot_t(da, b) + dot_t(db, a))
        g = dot_t(da, ra) + (dot_t(da, rb) + dot_t(db, ra))
        at = cols[:, levels + l : levels + l + 1]
        stats.append(lane_sum(jnp.where(lane == at, g, 0.0)))
    stat[...] = pack(stats)
    offset = 0.5 * (stats[levels] + stats[0])
    weight, kept, columns = level_step(
        0, levels, offset, proj, cols, member, sq, [], [], scale
    )
    out[...] = weight
    state[...] = jnp.zeros(state.shape, F32)
    state[0:1, :] = sq
    state[1:2, :] = kept[0][0]
    state[2:3, :] = kept[0][1]
    emit(columns, small, shared, n)


def level_kernel(got, proj, stat, before, counts, state, cols, member, *refs, l, levels, n, scale):
    small, shared, state_out, counts_out, out = refs
    splits = proj.shape[1]
    total = got[0]
    for i in range(1, n):
        total = total + got[i]
    fill = jnp.zeros((LANES - 8, splits), F32)
    down = jnp.transpose(jnp.concatenate([total, fill], axis=0))
    counts_out[...] = counts[...]
    counts_out[2 * (l - 1) : 2 * l, :] = 1.0 / (total[0:2, :] + 1.0)
    lane = iota((splits, splits), 1)

    def lookup(k):
        def run(half, odd):
            value = jnp.where(
                odd > 0, counts_out[2 * k + 1 : 2 * k + 2, :], counts_out[2 * k : 2 * k + 1, :]
            )
            return lane_sum(jnp.where(lane == half, value, 0.0))

        return run

    lookups = [lookup(k) for k in range(l)]
    half, odd, _ = ancestor(cols, levels, l, l - 1)
    inverse = lookups[l - 1](half, odd)
    root = stat[:, levels + l : levels + l + 1]
    dots = (down[:, 4:5] + before[:, 5:6] * root) * inverse
    offset = 0.5 * (dots + stat[:, l : l + 1])
    kept = [(state[1 + 2 * k : 2 + 2 * k, :], state[2 + 2 * k : 3 + 2 * k, :]) for k in range(l)]
    weight, kept, columns = level_step(
        l, levels, offset, proj, cols, member, state[0:1, :], kept, lookups, scale
    )
    out[...] = weight
    state_out[...] = state[...]
    state_out[1 + 2 * l : 2 + 2 * l, :] = kept[l][0]
    state_out[2 + 2 * l : 3 + 2 * l, :] = kept[l][1]
    columns = columns + [jnp.zeros((splits, 1), F32)] * (6 - len(columns)) + [inverse]
    emit(columns, small, shared, n)


def sums_kernel(place, nodes, *refs, l, levels, lead, per, own, clusters_rows):
    high, low, delta, mean, state, cols, small, before = refs[:8]
    outs = refs[8 : 8 + lead]
    total, scratch = refs[8 + lead :]
    rows, width = high.shape
    splits = delta.shape[1]
    number = iota((splits, rows), 0).astype(F32)
    index = state[1 + 2 * l : 2 + 2 * l, :]
    first = state[2 + 2 * l : 3 + 2 * l, :]
    chosen = number == index
    a, b = high[...], low[...]
    for j, f in enumerate((first, 1.0 - first)):
        wa, wb = split2(jnp.where(chosen, f, 0.0))
        scratch[:, j * width : (j + 1) * width] = dot(wa, a) + (dot(wa, b) + dot(wb, a))
    at = slice(2 * width, 3 * width)

    def move(s, carry):
        node = nodes[s]
        if l:
            value = before[lax.rem(node, 2), pl.ds(lax.div(node, 2), 1), :]
        else:
            value = before[pl.ds(node, 1), :]
        scratch[pl.ds(s, 1), at] = value
        return carry

    lax.fori_loop(0, splits, move, 0, unroll=8)
    if l:
        factor = small[:, 6:7]
    else:
        factor = jnp.where(place[2] == 0, 1.0, 0.0)
    mid = 0.5 * (scratch[:, at] * factor + mean[l])
    scratch[:, at] = mid
    half = 0.5 * delta[l]
    total[0] = scratch[:, 0:width] + (mid + half)
    total[1] = scratch[:, width : 2 * width] + (mid - half)
    scratch[:, 3 * width :] = small[...]
    to_blocks(scratch, outs, place[0], own, per)


def finish_kernel(*refs, levels):
    sums = refs[:levels]
    delta, out = refs[levels:]
    own = out.shape[0] // 2
    width = out.shape[1] - LANES
    spread = []
    for l in range(levels):
        mid = sums[l][:, 2 * width : 3 * width]
        half = 0.5 * delta[:, l * width : (l + 1) * width]
        for j in range(2):
            s = sums[l][:, j * width : (j + 1) * width]
            count = sums[l][:, 3 * width + j : 3 * width + j + 1]
            energy = sums[l][:, 3 * width + 2 + j : 3 * width + 3 + j]
            centre = (s + (mid + half if j == 0 else mid - half)) / (count + 1.0)
            error = (
                energy - 2.0 * lane_sum(centre * s) + count * lane_sum(centre * centre)
            )
            spread.append(error / ((count + 1.0) * width))
            if l + 1 == levels:
                for i in range(own):
                    out[2 * i + j : 2 * i + j + 1, :width] = centre[i : i + 1, :]
    out[:own, width:] = pack(spread)
    out[own:, width:] = jnp.zeros((own, LANES), F32)


def place_kernel(place, *refs, levels, lead, per, own):
    pieces = refs[:lead]
    centre, spread, scratch = refs[lead:]
    splits, width = scratch.shape[0], centre.shape[1]
    for j, piece in enumerate(pieces):
        for t in range(per):
            at = (place[0] ^ (j * per + t)) * own
            centre[pl.ds(pl.multiple_of(2 * at, 8), 2 * own), :] = piece[t, :, :width]
            scratch[pl.ds(pl.multiple_of(at, 8), own), :] = piece[t, :own, width:]
    across = jnp.transpose(scratch[...])[:8, :]
    a = across.astype(BF16)
    rest = across - a.astype(F32)
    b = rest.astype(BF16)
    c = (rest - b.astype(F32)).astype(BF16)
    total = jnp.zeros((8, 2 * splits), F32)
    outs = []
    for j in range(2):
        hot = jnp.where(
            iota((splits, 2 * splits), 1) == 2 * iota((splits, 2 * splits), 0) + j, 1.0, 0.0
        ).astype(BF16)
        outs.append(dot(a, hot) + (dot(b, hot) + dot(c, hot)))
    for l in range(levels):
        spread[l : l + 1, :] = outs[0][2 * l : 2 * l + 1, :] + outs[1][2 * l + 1 : 2 * l + 2, :]


def on_device(embeddings, root_centroids, member_ids, split_order, seed_rows):
    rows, width = embeddings.shape
    levels, splits = seed_rows.shape[:2]
    comm = Comm(lax.axis_size(AXES), splits // 8)
    n, lead = comm.n, comm.lead
    own = splits // comm.blocks
    per = comm.blocks // lead
    payload = levels * width + LANES
    scale = 0.5 / (float(width) ** 0.5)
    first_row = comm.me * rows
    place = jnp.stack([comm.block, first_row, comm.me]).astype(jnp.int32)
    smem = pl.BlockSpec(memory_space=pltpu.SMEM)
    vmem = pl.BlockSpec(memory_space=pltpu.VMEM)
    piece = jax.ShapeDtypeStruct((per, own, payload), F32)
    geometry = dict(lead=lead, per=per, own=own)

    def struct(shape, dtype=F32):
        return jax.ShapeDtypeStruct(shape, dtype)

    def call(kernel, name, outs, scalars, args, scratch=()):
        return pl.pallas_call(
            kernel,
            name=name,
            out_shape=outs,
            in_specs=[smem] * len(scalars) + [vmem] * len(args),
            out_specs=[vmem] * len(outs),
            scratch_shapes=[pltpu.VMEM(s, F32) for s in scratch],
            compiler_params=pltpu.CompilerParams(vmem_limit_bytes=60 * 1024 * 1024),
        )(*scalars, *args)

    *sent, high, low, delta, mean = call(
        functools.partial(pick_kernel, levels=levels, **geometry),
        "pick",
        [piece] * lead
        + [struct((rows, width), BF16)] * 2
        + [struct((levels, splits, width))] * 2,
        [place],
        [seed_rows, embeddings],
        [(splits, payload)],
    )

    order = split_order[:, :splits]
    local = seed_rows.reshape(levels, 2 * splits) - first_row
    chain, root_at = [], []
    for l in range(levels):
        node = order[l]
        found = []
        for k in range(l - 1, -1, -1):
            found.append([node // 2, node % 2, jnp.take(local[k], node)])
            node = jnp.take(order[k], node // 2)
        root_at.append(node)
        for entry in found[::-1]:
            chain += entry
    cols = jnp.stack([order[l] for l in range(levels)] + root_at + chain, axis=1)

    delta_own = comm.reduce_scatter(sent)
    pieces = comm.all_gather(delta_own)
    proj, stat, small, shared, state, weight = call(
        functools.partial(
            project_kernel, levels=levels, n=n, scale=scale, **geometry
        ),
        "project",
        [
            struct((levels, splits, rows)),
            struct((splits, LANES)),
            struct((splits, LANES)),
            struct((n, 8, splits)),
            struct((8, rows)),
            struct((1, rows)),
        ],
        [place],
        [*pieces, high, low, embeddings, root_centroids, cols, member_ids],
        [(splits, payload)],
    )
    weights_out = [weight]
    counts = jnp.zeros((8, splits), F32)
    before = root_centroids
    sums_own = []
    for l in range(levels):
        if l:
            got = comm.share(shared)
            small, shared, state, counts, weight = call(
                functools.partial(level_kernel, l=l, levels=levels, n=n, scale=scale),
                f"level{l}",
                [
                    struct((splits, LANES)),
                    struct((n, 8, splits)),
                    struct((8, rows)),
                    struct((8, splits)),
                    struct((1, rows)),
                ],
                [],
                [got, proj, stat, small, counts, state, cols, member_ids],
            )
            weights_out.append(weight)
        *sent, before = call(
            functools.partial(
                sums_kernel, l=l, levels=levels, clusters_rows=2 * splits, **geometry
            ),
            f"sums{l}",
            [piece] * lead + [struct((2, splits, width))],
            [place, order[l]],
            [high, low, delta, mean, state, cols, small, before],
            [(splits, payload)],
        )
        sums_own.append(comm.reduce_scatter(sent))
    (final,) = call(
        functools.partial(finish_kernel, levels=levels),
        "finish",
        [struct((2 * own, width + LANES))],
        [],
        [*sums_own, delta_own],
    )
    pieces = comm.all_gather(final)
    centre, spread = call(
        functools.partial(place_kernel, levels=levels, **geometry),
        "place",
        [struct((2 * splits, width)), struct((levels, 2 * splits))],
        [place],
        pieces,
        [(splits, LANES)],
    )
    return (centre, spread, jnp.concatenate(weights_out, axis=0))


def solution(mesh):
    in_specs = (P(AXES, None), P(), P(None, AXES), P(), P())
    out_specs = (P(), P(), P(None, AXES))
    return jax.shard_map(
        on_device, mesh=mesh, in_specs=in_specs, out_specs=out_specs, check_vma=False
    )
```

```python
import functools

import jax
import jax.numpy as jnp
from jax import lax
from jax.experimental import pallas as pl
from jax.experimental.pallas import tpu as pltpu
from jax.sharding import PartitionSpec as P

AXES = ("rows", "hosts")
LANES = 128
F32 = jnp.float32
BF16 = jnp.bfloat16


class Comm:
    def __init__(self, devices, most_blocks):
        self.n = devices
        self.me = lax.axis_index(AXES)
        bits = devices.bit_length() - 1
        assert 1 << bits == devices
        radices = [2] * (bits % 2) + [4] * (bits // 2)
        self.stages, self.extra = [], []
        self.blocks, stride, self.block = 1, 1, 0
        for radix in radices:
            if self.blocks * radix <= most_blocks:
                self.stages.append((radix, stride))
                self.block = self.block * radix + (self.me // stride) % radix
                self.blocks *= radix
            else:
                self.extra.append((radix, stride))
            stride *= radix
        self.lead = self.stages[0][0]

    def send(self, x, mask):
        return lax.ppermute(x, AXES, [(i, i ^ mask) for i in range(self.n)])

    def reduce_scatter(self, pieces):
        for step, (radix, stride) in enumerate(self.stages):
            if step:
                x = x.reshape((radix, x.shape[0] // radix) + x.shape[1:])
                pieces = [x[j] for j in range(radix)]
            got = [self.send(pieces[j], j * stride) for j in range(1, radix)]
            x = functools.reduce(jnp.add, got, pieces[0])
        x = x[0]
        for radix, stride in self.extra:
            while radix > 1:
                x = x + self.send(x, stride)
                stride, radix = stride * 2, radix // 2
        return x

    def all_gather(self, x):
        x = x[None]
        for radix, stride in self.stages[::-1]:
            pieces = [x] + [self.send(x, j * stride) for j in range(1, radix)]
            if (radix, stride) != self.stages[0]:
                x = jnp.concatenate(pieces)
        return pieces

    def share(self, x):
        return lax.all_to_all(x, AXES, 0, 0, tiled=True)


def dot(a, b):
    return lax.dot_general(a, b, (((1,), (0,)), ((), ())), preferred_element_type=F32)


def dot_t(a, b):
    return lax.dot_general(a, b, (((1,), (1,)), ((), ())), preferred_element_type=F32)


def split2(x):
    high = x.astype(BF16)
    return high, (x - high.astype(F32)).astype(BF16)


def iota(shape, axis):
    return lax.broadcasted_iota(jnp.int32, shape, axis)


def lane_sum(x):
    return jnp.sum(x, axis=1, keepdims=True)


def pack(columns):
    rows = columns[0].shape[0]
    lane = iota((rows, LANES), 1)
    out = jnp.zeros((rows, LANES), F32)
    for q, c in enumerate(columns):
        out = jnp.where(lane == q, c, out)
    return out


def to_blocks(scratch, outs, block, own, per):
    for j, out in enumerate(outs):
        for t in range(per):
            at = (block ^ (j * per + t)) * own
            out[t] = scratch[pl.ds(pl.multiple_of(at, 8), own), :]


def lanes(ref, l, width):
    return ref[:, l * width : (l + 1) * width]


def columns_of(rows):
    fill = jnp.zeros((LANES - rows.shape[0], rows.shape[1]), F32)
    return jnp.transpose(jnp.concatenate([rows, fill], axis=0))


def seed_columns(seeds, first_row):
    levels = seeds.shape[0]
    rows = [seeds[l].astype(F32) - first_row for l in range(levels)]
    return rows, columns_of(jnp.concatenate(rows, axis=0))


def halves_hot(found, row, l):
    hot0 = jnp.where(found[:, 2 * l : 2 * l + 1] == row, 0.5, 0.0)
    hot1 = jnp.where(found[:, 2 * l + 1 : 2 * l + 2] == row, 0.5, 0.0)
    return hot0, hot1


def pick_kernel(place, seeds, emb, *refs, levels, lead, per, own):
    outs = refs[:lead]
    high, low, squares, scratch = refs[lead:]
    rows, width = emb.shape
    splits = seeds.shape[2]
    e = emb[...]
    a, b = split2(e)
    high[...] = a
    low[...] = b
    column = lane_sum(e * e)
    sq = jnp.transpose(jnp.broadcast_to(column, (rows, LANES)))[0:1, :]
    squares[...] = sq
    _, found = seed_columns(seeds, place[1].astype(F32))
    row = iota((splits, rows), 1).astype(F32)
    bs = []
    for l in range(levels):
        hot0, hot1 = halves_hot(found, row, l)
        hot = hot0 - hot1
        d = hot.astype(BF16)
        scratch[:, l * width : (l + 1) * width] = dot(d, a) + dot(d, b)
        bs.append(0.5 * lane_sum(hot * sq))
    scratch[:, levels * width :] = pack(bs)
    to_blocks(scratch, outs, place[0], own, per)


def tables_kernel(place, seeds, order, root, high, low, cols, *refs, levels):
    means, deltas, roots = refs[:levels], refs[levels : 2 * levels], refs[2 * levels :]
    rows, width = high.shape
    splits = seeds.shape[2]
    seed_rows, found = seed_columns(seeds, place[1].astype(F32))
    order_rows = order[...][:, :splits].astype(F32)
    order_cols = columns_of(order_rows)
    row = iota((splits, rows), 1).astype(F32)
    lane = iota((splits, splits), 1).astype(F32)
    cluster = iota((splits, root.shape[0]), 1).astype(F32)
    a, b = high[...], low[...]
    ra, rb = split2(root[...])
    chain, root_at = [], []
    for l in range(levels):
        node = order_cols[:, l : l + 1]
        entry = []
        for k in range(l - 1, -1, -1):
            half = jnp.floor(node * 0.5)
            odd = node - 2.0 * half
            value = jnp.where(odd > 0, seed_rows[k][1:2, :], seed_rows[k][0:1, :])
            hit = lane == half
            entry.append([half, odd, lane_sum(jnp.where(hit, value, 0.0))])
            node = lane_sum(jnp.where(hit, order_rows[k : k + 1, :], 0.0))
        for e in entry[::-1]:
            chain += e
        root_at.append(node)
        hot = jnp.where(cluster == node, 1.0, 0.0).astype(BF16)
        roots[l][...] = dot(hot, ra) + dot(hot, rb)
        hot0, hot1 = halves_hot(found, row, l)
        d, m = (hot0 - hot1).astype(BF16), (hot0 + hot1).astype(BF16)
        means[l][...] = dot(m, a) + dot(m, b)
        deltas[l][...] = dot(d, a) + dot(d, b)
    cols[...] = pack([order_cols[:, l : l + 1] for l in range(levels)] + root_at + chain)


def level_step(l, levels, offset, proj, ahead, cols, member, sq, rows_in, lookups, scale):
    splits, rows = proj.shape
    chosen = cols[:, l : l + 1] == member[l : l + 1, :].astype(F32)
    part = jnp.where(chosen, proj - offset, 0.0)
    gap = 2.0 * jnp.sum(part, axis=0, keepdims=True)
    inside = jnp.sum(jnp.where(chosen, 1.0, 0.0), axis=0, keepdims=True)
    first = jax.nn.sigmoid(gap * scale)
    number = iota((splits, rows), 0).astype(F32)
    index = jnp.sum(jnp.where(chosen, number + 1.0, 0.0), axis=0, keepdims=True) - 1.0
    w0 = jnp.where(chosen, first, 0.0)
    w1 = jnp.where(chosen, 1.0 - first, 0.0)
    columns = [lane_sum(w0), lane_sum(w1), lane_sum(w0 * sq), lane_sum(w1 * sq)]
    rows_out = rows_in + [(index, first)]
    if l + 1 < levels:
        row = iota((splits, rows), 1).astype(F32)
        coef = jnp.ones((splits, 1), F32)
        total = jnp.zeros((splits, 1), F32)
        for k in range(l, -1, -1):
            half, odd, seed = ancestor(cols, levels, l + 1, k)
            if k < l:
                coef = coef * lookups[k](half, odd)
            at, f = rows_out[k]
            w = jnp.where(at == half, jnp.where(odd > 0, 1.0 - f, f), 0.0)
            w = w + jnp.where(row == seed, 0.5, 0.0)
            total = total + coef * lane_sum(w * ahead)
            coef = 0.5 * coef
        columns += [total, coef]
    return first * inside, rows_out, columns


def ancestor(cols, levels, l, k):
    at = 2 * levels + 3 * (l * (l - 1) // 2 + k)
    return cols[:, at : at + 1], cols[:, at + 1 : at + 2], cols[:, at + 2 : at + 3]


def emit(columns, small, shared):
    packed = pack(columns)
    small[...] = packed
    if shared is not None:
        across = jnp.transpose(packed)[:8, :]
        for i in range(shared.shape[0]):
            shared[i] = across


def delta_of(pieces, block, own, per, lo, hi, scratch):
    for j, piece in enumerate(pieces):
        for t in range(per):
            at = (block ^ (j * per + t)) * own
            scratch[pl.ds(pl.multiple_of(at, 8), own), :] = piece[t, :, lo:hi]


def project(da, db, a, b):
    return dot_t(da, a) + (dot_t(da, b) + dot_t(db, a))


def project_kernel(place, *refs, levels, lead, per, own, scale):
    pieces = refs[:lead]
    high, low, squares, root0, root1, cols, member = refs[lead : lead + 7]
    proj, stat, small, shared, state, out, scratch, extra = refs[lead + 7 :]
    width = high.shape[1]
    delta_of(pieces, place[0], own, per, levels * width, levels * width + LANES, extra)
    stats = [extra[:, l : l + 1] for l in range(levels)]
    a, b = high[...], low[...]
    made = []
    for l, root in enumerate((root0, root1)):
        delta_of(pieces, place[0], own, per, l * width, (l + 1) * width, scratch)
        d = scratch[...]
        stats.append(lane_sum(d * root[...]))
        made.append(project(*split2(d), a, b))
    proj[...] = made[1]
    stat[...] = pack(stats)
    sq = squares[...]
    offset = 0.5 * (stats[levels] + stats[0])
    weight, kept, columns = level_step(
        0, levels, offset, made[0], made[1], cols, member, sq, [], [], scale
    )
    out[...] = weight
    state[...] = jnp.zeros(state.shape, F32)
    state[0:1, :] = sq
    state[1:2, :] = kept[0][0]
    state[2:3, :] = kept[0][1]
    emit(columns, small, shared)


def ahead_kernel(place, *refs, l, levels, lead, per, own):
    pieces = refs[:lead]
    high, low, root, proj, stat, scratch = refs[lead:]
    width = high.shape[1]
    delta_of(pieces, place[0], own, per, l * width, (l + 1) * width, scratch)
    d = scratch[...]
    stat[...] = jnp.broadcast_to(lane_sum(d * root[...]), stat.shape)
    proj[...] = project(*split2(d), high[...], low[...])


def level_kernel(*refs, l, levels, n, scale):
    refs = list(refs)
    got, proj = refs.pop(0), refs.pop(0)
    ahead = refs.pop(0) if l + 1 < levels else None
    stat, root_stat, before, state, cols, member = (refs.pop(0) for _ in range(6))
    counts = refs.pop(0) if l > 1 else None
    small, state_out, counts_out, out = (refs.pop(0) for _ in range(4))
    shared = refs.pop(0) if l + 1 < levels else None
    splits = proj.shape[0]
    total = got[0]
    for i in range(1, n):
        total = total + got[i]
    down = columns_of(total)
    counts_out[...] = jnp.zeros(counts_out.shape, F32) if counts is None else counts[...]
    counts_out[2 * (l - 1) : 2 * l, :] = 1.0 / (total[0:2, :] + 1.0)
    lane = iota((splits, splits), 1).astype(F32)

    def lookup(k):
        def run(half, odd):
            value = jnp.where(
                odd > 0, counts_out[2 * k + 1 : 2 * k + 2, :], counts_out[2 * k : 2 * k + 1, :]
            )
            return lane_sum(jnp.where(lane == half, value, 0.0))

        return run

    lookups = [lookup(k) for k in range(l)]
    half, odd, _ = ancestor(cols, levels, l, l - 1)
    inverse = lookups[l - 1](half, odd)
    at = levels + 1 if l == 1 else 0
    root = root_stat[:, at : at + 1]
    dots = (down[:, 4:5] + before[:, 5:6] * root) * inverse
    offset = 0.5 * (dots + stat[:, l : l + 1])
    kept = [(state[1 + 2 * k : 2 + 2 * k, :], state[2 + 2 * k : 3 + 2 * k, :]) for k in range(l)]
    weight, kept, columns = level_step(
        l,
        levels,
        offset,
        proj[...],
        None if ahead is None else ahead[...],
        cols,
        member,
        state[0:1, :],
        kept,
        lookups,
        scale,
    )
    out[...] = weight
    state_out[...] = state[...]
    state_out[1 + 2 * l : 2 + 2 * l, :] = kept[l][0]
    state_out[2 + 2 * l : 3 + 2 * l, :] = kept[l][1]
    columns = columns + [jnp.zeros((splits, 1), F32)] * (6 - len(columns)) + [inverse]
    emit(columns, small, shared)


def sums_kernel(place, order, *refs, l, levels, lead, per, own):
    refs = list(refs)
    high, low, state, small = (refs.pop(0) for _ in range(4))
    more = l + 1 < levels
    if more:
        mean, delta, start = (refs.pop(0) for _ in range(3))
    later = [refs.pop(0) for _ in range(levels - 2)] if l == 0 else []
    outs = [refs.pop(0) for _ in range(lead)]
    carry_out = refs.pop(0) if l == 0 else None
    scratch = refs.pop(0)
    tables = refs.pop(0) if more else None
    rows, width = high.shape
    splits = small.shape[0]
    number = iota((splits, rows), 0).astype(F32)
    index = state[1 + 2 * l : 2 + 2 * l, :]
    first = state[2 + 2 * l : 3 + 2 * l, :]
    chosen = number == index
    a, b = high[...], low[...]
    for j, f in enumerate((first, 1.0 - first)):
        wa, wb = split2(jnp.where(chosen, f, 0.0))
        scratch[:, j * width : (j + 1) * width] = dot(wa, a) + (dot(wa, b) + dot(wb, a))
    at = 2
    if more:
        m = mean[...]
        if l:
            mid = 0.5 * (start[...] * small[:, 6:7] + m)
            if l == 1:
                scratch[:, at * width : (at + 1) * width] = mid
                at += 1
        else:
            mid = 0.5 * (start[...] * jnp.where(place[2] == 0, 1.0, 0.0) + m)
            scratch[:, at * width : (at + 1) * width] = m
            at += 1
        half = 0.5 * delta[...]
        tables[0] = lanes(scratch, 0, width) + (mid + half)
        tables[1] = lanes(scratch, 1, width) + (mid - half)
        first_lane = at * width

        def move(s, carry):
            node = order[l + 1, s]
            value = tables[lax.rem(node, 2), pl.ds(lax.div(node, 2), 1), :]
            if l:
                scratch[pl.ds(s, 1), first_lane : first_lane + width] = value
            else:
                carry_out[pl.ds(s, 1), :] = value
            return carry

        lax.fori_loop(0, splits, move, 0, unroll=8)
        if l:
            at += 1
    for ref in later:
        scratch[:, at * width : (at + 1) * width] = ref[...]
        at += 1
    scratch[:, at * width :] = small[...]
    to_blocks(scratch, outs, place[0], own, per)


def finish_kernel(place, *refs, levels):
    sums = refs[:levels]
    smalls = refs[levels : 2 * levels - 2]
    root, delta, out = refs[2 * levels - 2 :]
    own = out.shape[0] // 2
    width = out.shape[1] - LANES
    here = pl.ds(pl.multiple_of(place[0] * own, 8), own)
    spread = []
    for l in range(levels):
        if l == 0:
            mid = 0.5 * (lanes(sums[0], 2, width) + root[here, :])
        elif l == 1:
            mid = lanes(sums[1], 2, width)
        else:
            grown = lanes(sums[l - 1], 3 if l == 2 else 2, width)
            inverse = smalls[l - 2][here, 6:7]
            mid = 0.5 * (grown * inverse + lanes(sums[0], l + 1, width))
        half = 0.5 * lanes(delta, l, width)
        last = sums[l].shape[1] - LANES
        for j in range(2):
            s = lanes(sums[l], j, width)
            count = sums[l][:, last + j : last + j + 1]
            energy = sums[l][:, last + 2 + j : last + 3 + j]
            centre = (s + (mid + half if j == 0 else mid - half)) / (count + 1.0)
            error = (
                energy - 2.0 * lane_sum(centre * s) + count * lane_sum(centre * centre)
            )
            spread.append(error / ((count + 1.0) * width))
            if l + 1 == levels:
                for i in range(own):
                    out[2 * i + j : 2 * i + j + 1, :width] = centre[i : i + 1, :]
    out[:own, width:] = pack(spread)
    out[own:, width:] = jnp.zeros((own, LANES), F32)


def place_kernel(place, *refs, levels, lead, per, own):
    pieces = refs[:lead]
    centre, spread, scratch = refs[lead:]
    splits, width = scratch.shape[0], centre.shape[1]
    for j, piece in enumerate(pieces):
        for t in range(per):
            at = (place[0] ^ (j * per + t)) * own
            centre[pl.ds(pl.multiple_of(2 * at, 8), 2 * own), :] = piece[t, :, :width]
            scratch[pl.ds(pl.multiple_of(at, 8), own), :] = piece[t, :own, width:]
    across = jnp.transpose(scratch[...])[:8, :]
    a = across.astype(BF16)
    rest = across - a.astype(F32)
    b = rest.astype(BF16)
    c = (rest - b.astype(F32)).astype(BF16)
    total = jnp.zeros((8, 2 * splits), F32)
    outs = []
    for j in range(2):
        hot = jnp.where(
            iota((splits, 2 * splits), 1) == 2 * iota((splits, 2 * splits), 0) + j, 1.0, 0.0
        ).astype(BF16)
        outs.append(dot(a, hot) + (dot(b, hot) + dot(c, hot)))
    for l in range(levels):
        spread[l : l + 1, :] = outs[0][2 * l : 2 * l + 1, :] + outs[1][2 * l + 1 : 2 * l + 2, :]


def on_device(embeddings, root_centroids, member_ids, split_order, seed_rows):
    rows, width = embeddings.shape
    levels, splits = seed_rows.shape[:2]
    assert levels == 3
    comm = Comm(lax.axis_size(AXES), splits // 8)
    n, lead = comm.n, comm.lead
    own = splits // comm.blocks
    per = comm.blocks // lead
    scale = 0.5 / (float(width) ** 0.5)
    place = jnp.stack([comm.block, comm.me * rows, comm.me]).astype(jnp.int32)
    smem = pl.BlockSpec(memory_space=pltpu.SMEM)
    vmem = pl.BlockSpec(memory_space=pltpu.VMEM)
    geometry = dict(levels=levels, lead=lead, per=per, own=own)
    table = (splits, width)
    narrow = (splits, LANES)

    def struct(shape, dtype=F32):
        return jax.ShapeDtypeStruct(shape, dtype)

    def pieces_of(parts):
        return [struct((per, own, parts * width + LANES))] * lead

    def call(kernel, name, outs, scalars, args, scratch=(), limit=30):
        run = pl.pallas_call(
            kernel,
            name=name,
            out_shape=outs,
            in_specs=[smem] * len(scalars) + [vmem] * len(args),
            out_specs=[vmem] * len(outs),
            scratch_shapes=[pltpu.VMEM(s, F32) for s in scratch],
            compiler_params=pltpu.CompilerParams(vmem_limit_bytes=limit * 1024 * 1024),
        )
        return list(run(*scalars, *args))

    seeds = seed_rows.transpose(0, 2, 1)
    *sent, high, low, squares = call(
        functools.partial(pick_kernel, **geometry),
        "pick",
        pieces_of(levels) + [struct((rows, width), BF16)] * 2 + [struct((1, rows))],
        [place],
        [seeds, embeddings],
        [(splits, levels * width + LANES)],
    )
    cols, *rest = call(
        functools.partial(tables_kernel, levels=levels),
        "tables",
        [struct(narrow)] + [struct(table)] * (3 * levels),
        [place],
        [seeds, split_order, root_centroids, high, low],
    )
    means, deltas, roots = rest[:levels], rest[levels : 2 * levels], rest[2 * levels :]
    delta_own = comm.reduce_scatter(sent)
    pieces = comm.all_gather(delta_own)
    proj, stat, small, shared, state, weight = call(
        functools.partial(project_kernel, scale=scale, **geometry),
        "project",
        [
            struct((splits, rows)),
            struct(narrow),
            struct(narrow),
            struct((n, 8, splits)),
            struct((8, rows)),
            struct((1, rows)),
        ],
        [place],
        [*pieces, high, low, squares, roots[0], roots[1], cols, member_ids],
        [table, narrow],
    )
    projs, root_stats = [None, proj], [None, stat]
    for l in range(2, levels):
        made, root_stat = call(
            functools.partial(ahead_kernel, l=l, **geometry),
            f"ahead{l}",
            [struct((splits, rows)), struct(narrow)],
            [place],
            [*pieces, high, low, roots[l]],
            [table],
        )
        projs.append(made)
        root_stats.append(root_stat)
    weights_out = [weight]
    counts, start = [], roots[0]
    sums_own, smalls = [], []
    for l in range(levels):
        more = l + 1 < levels
        if l:
            outs = [
                struct(narrow),
                struct((8, rows)),
                struct((8, splits)),
                struct((1, rows)),
            ]
            small, state, count, weight, *shared = call(
                functools.partial(level_kernel, l=l, levels=levels, n=n, scale=scale),
                f"level{l}",
                outs + [struct((n, 8, splits))] * more,
                [],
                [got, *projs[l : l + 2], stat, root_stats[l], small, state, cols, member_ids]
                + counts,
            )
            counts = [count]
            weights_out.append(weight)
            if l > 1:
                smalls.append(small)
            shared = shared[0] if more else None
        if more:
            got = comm.share(shared)
        args = [high, low, state, small]
        if more:
            args += [means[l], deltas[l], start]
        if l == 0:
            args += means[2:]
        parts = 2 + (levels - 1 if l == 0 else (l == 1) + more)
        out = call(
            functools.partial(sums_kernel, l=l, **geometry),
            f"sums{l}",
            pieces_of(parts) + [struct(table)] * (l == 0),
            [place, split_order],
            args,
            [(splits, parts * width + LANES)] + [(2, splits, width)] * more,
        )
        if l == 0:
            start = out.pop()
        sums_own.append(comm.reduce_scatter(out))
    (final,) = call(
        functools.partial(finish_kernel, levels=levels),
        "finish",
        [struct((2 * own, width + LANES))],
        [place],
        [*sums_own, *smalls, roots[0], delta_own],
    )
    pieces = comm.all_gather(final)
    centre, spread = call(
        functools.partial(place_kernel, **geometry),
        "place",
        [struct((2 * splits, width)), struct((levels, 2 * splits))],
        [place],
        pieces,
        [narrow],
    )
    return (centre, spread, jnp.concatenate(weights_out, axis=0))


def solution(mesh):
    in_specs = (P(AXES, None), P(), P(None, AXES), P(), P())
    out_specs = (P(), P(), P(None, AXES))
    return jax.shard_map(
        on_device, mesh=mesh, in_specs=in_specs, out_specs=out_specs, check_vma=False
    )
```

```python
import functools

import jax
import jax.numpy as jnp
from jax import lax
from jax.experimental import pallas as pl
from jax.experimental.pallas import tpu as pltpu
from jax.sharding import PartitionSpec as P

AXES = ("rows", "hosts")
LANES = 128
F32 = jnp.float32
BF16 = jnp.bfloat16


class Comm:
    def __init__(self, devices, most_blocks):
        self.n = devices
        self.me = lax.axis_index(AXES)
        bits = devices.bit_length() - 1
        assert 1 << bits == devices
        radices = [2] * (bits % 2) + [4] * (bits // 2)
        self.stages, self.extra = [], []
        self.blocks, stride, self.block = 1, 1, 0
        for radix in radices:
            if self.blocks * radix <= most_blocks:
                self.stages.append((radix, stride))
                self.block = self.block * radix + (self.me // stride) % radix
                self.blocks *= radix
            else:
                self.extra.append((radix, stride))
            stride *= radix
        self.lead = self.stages[0][0]

    def send(self, x, mask):
        return lax.ppermute(x, AXES, [(i, i ^ mask) for i in range(self.n)])

    def spread_out(self, x, step):
        if step == 0:
            return x
        radix = self.stages[step][0]
        x = x.reshape((radix, x.shape[0] // radix) + x.shape[1:])
        return [x[j] for j in range(radix)]

    def scatter_send(self, pieces, step):
        stride = self.stages[step][1]
        return [self.send(pieces[j], j * stride) for j in range(1, len(pieces))]

    def add_up(self, pieces, got):
        return functools.reduce(jnp.add, got, pieces[0])

    def scatter_rest(self, x, step):
        for at in range(step, len(self.stages)):
            pieces = self.spread_out(x, at)
            x = self.add_up(pieces, self.scatter_send(pieces, at))
        x = x[0]
        for radix, stride in self.extra:
            while radix > 1:
                x = x + self.send(x, stride)
                stride, radix = stride * 2, radix // 2
        return x

    def gather_send(self, x, step):
        radix, stride = self.stages[step]
        return [self.send(x, j * stride) for j in range(1, radix)]

    def all_reduce(self, x):
        for radix, stride in self.stages + self.extra:
            got = [self.send(x, j * stride) for j in range(1, radix)]
            x = functools.reduce(jnp.add, got, x)
        return x


def tie(*trees):
    return lax.optimization_barrier(trees)


def dot(a, b):
    return lax.dot_general(a, b, (((1,), (0,)), ((), ())), preferred_element_type=F32)


def dot_t(a, b):
    return lax.dot_general(a, b, (((1,), (1,)), ((), ())), preferred_element_type=F32)


def split2(x):
    high = x.astype(BF16)
    return high, (x - high.astype(F32)).astype(BF16)


def iota(shape, axis):
    return lax.broadcasted_iota(jnp.int32, shape, axis)


def lane_sum(x):
    return jnp.sum(x, axis=1, keepdims=True)


def pack(columns):
    rows = columns[0].shape[0]
    lane = iota((rows, LANES), 1)
    out = jnp.zeros((rows, LANES), F32)
    for q, c in enumerate(columns):
        out = jnp.where(lane == q, c, out)
    return out


def to_blocks(scratch, outs, block, own, per):
    for j, out in enumerate(outs):
        for t in range(per):
            at = (block ^ (j * per + t)) * own
            out[t] = scratch[pl.ds(pl.multiple_of(at, 8), own), :]


def lanes(ref, l, width):
    return ref[:, l * width : (l + 1) * width]


def columns_of(rows):
    fill = jnp.zeros((LANES - rows.shape[0], rows.shape[1]), F32)
    return jnp.transpose(jnp.concatenate([rows, fill], axis=0))


def seed_columns(seeds, first_row):
    levels = seeds.shape[0]
    rows = [seeds[l].astype(F32) - first_row for l in range(levels)]
    return rows, columns_of(jnp.concatenate(rows, axis=0))


def halves_hot(found, row, l):
    hot0 = jnp.where(found[:, 2 * l : 2 * l + 1] == row, 0.5, 0.0)
    hot1 = jnp.where(found[:, 2 * l + 1 : 2 * l + 2] == row, 0.5, 0.0)
    return hot0, hot1


def pick_kernel(place, seeds, emb, *refs, levels, lead, per, own):
    outs = refs[:lead]
    high, low, squares, scratch = refs[lead:]
    rows, width = emb.shape
    splits = seeds.shape[2]
    e = emb[...]
    a, b = split2(e)
    high[...] = a
    low[...] = b
    column = lane_sum(e * e)
    sq = jnp.transpose(jnp.broadcast_to(column, (rows, LANES)))[0:1, :]
    squares[...] = sq
    _, found = seed_columns(seeds, place[1].astype(F32))
    row = iota((splits, rows), 1).astype(F32)
    bs = []
    for l in range(levels):
        hot0, hot1 = halves_hot(found, row, l)
        hot = hot0 - hot1
        d = hot.astype(BF16)
        scratch[:, l * width : (l + 1) * width] = dot(d, a) + dot(d, b)
        bs.append(0.5 * lane_sum(hot * sq))
    scratch[:, levels * width :] = pack(bs)
    to_blocks(scratch, outs, place[0], own, per)


def tables_kernel(place, seeds, order, root, cols, *roots, levels):
    splits = seeds.shape[2]
    seed_rows, _ = seed_columns(seeds, place[1].astype(F32))
    order_rows = order[...][:, :splits].astype(F32)
    order_cols = columns_of(order_rows)
    lane = iota((splits, splits), 1).astype(F32)
    cluster = iota((splits, root.shape[0]), 1).astype(F32)
    ra, rb = split2(root[...])
    chain, root_at = [], []
    for l in range(levels):
        node = order_cols[:, l : l + 1]
        entry = []
        for k in range(l - 1, -1, -1):
            half = jnp.floor(node * 0.5)
            odd = node - 2.0 * half
            value = jnp.where(odd > 0, seed_rows[k][1:2, :], seed_rows[k][0:1, :])
            hit = lane == half
            entry.append([half, odd, lane_sum(jnp.where(hit, value, 0.0))])
            node = lane_sum(jnp.where(hit, order_rows[k : k + 1, :], 0.0))
        for e in entry[::-1]:
            chain += e
        root_at.append(node)
        hot = jnp.where(cluster == node, 1.0, 0.0).astype(BF16)
        roots[l][...] = dot(hot, ra) + dot(hot, rb)
    cols[...] = pack([order_cols[:, l : l + 1] for l in range(levels)] + root_at + chain)


def means_kernel(place, seeds, order, member, high, low, *refs, levels, lead, per, own):
    outs = refs[:lead]
    means, deltas, wholes = (refs[lead + i * (levels - 1) :][: levels - 1] for i in range(3))
    scratch = refs[lead + 3 * (levels - 1)]
    rows, width = high.shape
    splits = seeds.shape[2]
    _, found = seed_columns(seeds, place[1].astype(F32))
    order_cols = columns_of(order[...][:, :splits].astype(F32))
    row = iota((splits, rows), 1).astype(F32)
    a, b = high[...], low[...]
    for l in range(levels):
        hot0, hot1 = halves_hot(found, row, l)
        m = (hot0 + hot1).astype(BF16)
        mean = dot(m, a) + dot(m, b)
        chosen = order_cols[:, l : l + 1] == member[l : l + 1, :].astype(F32)
        c = jnp.where(chosen, 1.0, 0.0).astype(BF16)
        whole = dot(c, a) + dot(c, b)
        scratch[:, l * width : (l + 1) * width] = mean
        scratch[:, (levels + l) * width : (levels + l + 1) * width] = whole
        if l + 1 < levels:
            d = (hot0 - hot1).astype(BF16)
            means[l][...] = mean
            deltas[l][...] = dot(d, a) + dot(d, b)
            wholes[l][...] = whole
    to_blocks(scratch, outs, place[0], own, per)


def level_step(l, levels, offset, proj, ahead, cols, member, sq, rows_in, lookups, scale):
    splits, rows = proj.shape
    chosen = cols[:, l : l + 1] == member[l : l + 1, :].astype(F32)
    part = jnp.where(chosen, proj - offset, 0.0)
    gap = 2.0 * jnp.sum(part, axis=0, keepdims=True)
    inside = jnp.sum(jnp.where(chosen, 1.0, 0.0), axis=0, keepdims=True)
    first = jax.nn.sigmoid(gap * scale)
    number = iota((splits, rows), 0).astype(F32)
    index = jnp.sum(jnp.where(chosen, number + 1.0, 0.0), axis=0, keepdims=True) - 1.0
    w0 = jnp.where(chosen, first, 0.0)
    w1 = jnp.where(chosen, 1.0 - first, 0.0)
    columns = [lane_sum(w0), lane_sum(w1), lane_sum(w0 * sq), lane_sum(w1 * sq)]
    rows_out = rows_in + [(index, first)]
    if l + 1 < levels:
        row = iota((splits, rows), 1).astype(F32)
        coef = jnp.ones((splits, 1), F32)
        total = jnp.zeros((splits, 1), F32)
        for k in range(l, -1, -1):
            half, odd, seed = ancestor(cols, levels, l + 1, k)
            if k < l:
                coef = coef * lookups[k](half, odd)
            at, f = rows_out[k]
            w = jnp.where(at == half, jnp.where(odd > 0, 1.0 - f, f), 0.0)
            w = w + jnp.where(row == seed, 0.5, 0.0)
            total = total + coef * lane_sum(w * ahead)
            coef = 0.5 * coef
        columns += [total, coef]
    return first * inside, rows_out, columns


def ancestor(cols, levels, l, k):
    at = 2 * levels + 3 * (l * (l - 1) // 2 + k)
    return cols[:, at : at + 1], cols[:, at + 1 : at + 2], cols[:, at + 2 : at + 3]


def emit(columns, small, across):
    packed = pack(columns)
    small[...] = packed
    if across is not None:
        across[...] = jnp.transpose(packed)[:8, :]


def delta_of(pieces, block, own, per, lo, hi, scratch):
    for j, piece in enumerate(pieces):
        for t in range(per):
            at = (block ^ (j * per + t)) * own
            scratch[pl.ds(pl.multiple_of(at, 8), own), :] = piece[t, :, lo:hi]


def project(da, db, a, b):
    return dot_t(da, a) + (dot_t(da, b) + dot_t(db, a))


def project_kernel(place, *refs, levels, lead, per, own, scale):
    pieces = refs[:lead]
    high, low, squares, root0, root1, cols, member = refs[lead : lead + 7]
    proj, stat, small, shared, state, out, scratch, extra = refs[lead + 7 :]
    width = high.shape[1]
    delta_of(pieces, place[0], own, per, levels * width, levels * width + LANES, extra)
    stats = [extra[:, l : l + 1] for l in range(levels)]
    a, b = high[...], low[...]
    made = []
    for l, root in enumerate((root0, root1)):
        delta_of(pieces, place[0], own, per, l * width, (l + 1) * width, scratch)
        d = scratch[...]
        stats.append(lane_sum(d * root[...]))
        made.append(project(*split2(d), a, b))
    proj[...] = made[1]
    stat[...] = pack(stats)
    sq = squares[...]
    offset = 0.5 * (stats[levels] + stats[0])
    weight, kept, columns = level_step(
        0, levels, offset, made[0], made[1], cols, member, sq, [], [], scale
    )
    out[...] = weight
    state[...] = jnp.zeros(state.shape, F32)
    state[0:1, :] = sq
    state[1:2, :] = kept[0][0]
    state[2:3, :] = kept[0][1]
    emit(columns, small, shared)


def ahead_kernel(place, *refs, l, levels, lead, per, own):
    pieces = refs[:lead]
    high, low, root, proj, stat, scratch = refs[lead:]
    width = high.shape[1]
    delta_of(pieces, place[0], own, per, l * width, (l + 1) * width, scratch)
    d = scratch[...]
    stat[...] = jnp.broadcast_to(lane_sum(d * root[...]), stat.shape)
    proj[...] = project(*split2(d), high[...], low[...])


def level_kernel(*refs, l, levels, scale):
    refs = list(refs)
    got, proj = refs.pop(0), refs.pop(0)
    ahead = refs.pop(0) if l + 1 < levels else None
    stat, root_stat, before, state, cols, member = (refs.pop(0) for _ in range(6))
    counts = refs.pop(0) if l > 1 else None
    small, state_out, counts_out, out = (refs.pop(0) for _ in range(4))
    shared = refs.pop(0) if l + 1 < levels else None
    splits = proj.shape[0]
    total = got[...]
    down = columns_of(total)
    counts_out[...] = jnp.zeros(counts_out.shape, F32) if counts is None else counts[...]
    counts_out[2 * (l - 1) : 2 * l, :] = 1.0 / (total[0:2, :] + 1.0)
    lane = iota((splits, splits), 1).astype(F32)

    def lookup(k):
        def run(half, odd):
            value = jnp.where(
                odd > 0, counts_out[2 * k + 1 : 2 * k + 2, :], counts_out[2 * k : 2 * k + 1, :]
            )
            return lane_sum(jnp.where(lane == half, value, 0.0))

        return run

    lookups = [lookup(k) for k in range(l)]
    half, odd, _ = ancestor(cols, levels, l, l - 1)
    inverse = lookups[l - 1](half, odd)
    at = levels + 1 if l == 1 else 0
    root = root_stat[:, at : at + 1]
    dots = (down[:, 4:5] + before[:, 5:6] * root) * inverse
    offset = 0.5 * (dots + stat[:, l : l + 1])
    kept = [(state[1 + 2 * k : 2 + 2 * k, :], state[2 + 2 * k : 3 + 2 * k, :]) for k in range(l)]
    weight, kept, columns = level_step(
        l,
        levels,
        offset,
        proj[...],
        None if ahead is None else ahead[...],
        cols,
        member,
        state[0:1, :],
        kept,
        lookups,
        scale,
    )
    out[...] = weight
    state_out[...] = state[...]
    state_out[1 + 2 * l : 2 + 2 * l, :] = kept[l][0]
    state_out[2 + 2 * l : 3 + 2 * l, :] = kept[l][1]
    columns = columns + [jnp.zeros((splits, 1), F32)] * (6 - len(columns)) + [inverse]
    emit(columns, small, shared)


def sums_kernel(place, order, *refs, l, levels, lead, per, own):
    refs = list(refs)
    more = l + 1 < levels
    high, low, state, small = (refs.pop(0) for _ in range(4))
    if more:
        whole, mean, delta, start = (refs.pop(0) for _ in range(4))
    outs = [refs.pop(0) for _ in range(lead)]
    carry_out = refs.pop(0) if l + 2 < levels else None
    scratch = refs.pop(0)
    tables = refs.pop(0) if more else None
    rows, width = high.shape
    splits = small.shape[0]
    number = iota((splits, rows), 0).astype(F32)
    index = state[1 + 2 * l : 2 + 2 * l, :]
    first = state[2 + 2 * l : 3 + 2 * l, :]
    a, b = high[...], low[...]
    wa, wb = split2(jnp.where(number == index, first, 0.0))
    sums = dot(wa, a) + (dot(wa, b) + dot(wb, a))
    scratch[:, :width] = sums
    if more:
        factor = small[:, 6:7] if l else jnp.where(place[2] == 0, 1.0, 0.0)
        mid = 0.5 * (start[...] * factor + mean[...])
        half = 0.5 * delta[...]
        tables[0] = sums + (mid + half)
        tables[1] = (whole[...] - sums) + (mid - half)

        def move(s, carry):
            node = order[l + 1, s]
            value = tables[lax.rem(node, 2), pl.ds(lax.div(node, 2), 1), :]
            scratch[pl.ds(s, 1), width : 2 * width] = value
            return carry

        lax.fori_loop(0, splits, move, 0, unroll=8)
        if carry_out is not None:
            carry_out[...] = scratch[:, width : 2 * width]
        scratch[:, 2 * width :] = small[...]
    else:
        scratch[:, width:] = small[...]
    to_blocks(scratch, outs, place[0], own, per)


def finish_kernel(place, *refs, levels):
    sums = refs[:levels]
    smalls = refs[levels : 2 * levels - 1]
    early, root, delta, out = refs[2 * levels - 1 :]
    own = out.shape[0] // 2
    width = out.shape[1] - LANES
    here = pl.ds(pl.multiple_of(place[0] * own, 8), own)
    spread = []
    for l in range(levels):
        if l:
            start = lanes(sums[l - 1], 1, width) * smalls[l - 1][here, 6:7]
        else:
            start = root[here, :]
        mid = 0.5 * (start + lanes(early, l, width))
        half = 0.5 * lanes(delta, l, width)
        last = sums[l].shape[1] - LANES
        for j in range(2):
            s = lanes(sums[l], 0, width)
            if j:
                s = lanes(early, levels + l, width) - s
            count = sums[l][:, last + j : last + j + 1]
            energy = sums[l][:, last + 2 + j : last + 3 + j]
            centre = (s + (mid + half if j == 0 else mid - half)) / (count + 1.0)
            error = (
                energy - 2.0 * lane_sum(centre * s) + count * lane_sum(centre * centre)
            )
            spread.append(error / ((count + 1.0) * width))
            if l + 1 == levels:
                for i in range(own):
                    out[2 * i + j : 2 * i + j + 1, :width] = centre[i : i + 1, :]
    out[:own, width:] = pack(spread)
    out[own:, width:] = jnp.zeros((own, LANES), F32)


def place_kernel(place, *refs, levels, lead, per, own):
    pieces = refs[:lead]
    centre, spread, scratch = refs[lead:]
    splits, width = scratch.shape[0], centre.shape[1]
    for j, piece in enumerate(pieces):
        for t in range(per):
            at = (place[0] ^ (j * per + t)) * own
            centre[pl.ds(pl.multiple_of(2 * at, 8), 2 * own), :] = piece[t, :, :width]
            scratch[pl.ds(pl.multiple_of(at, 8), own), :] = piece[t, :own, width:]
    across = jnp.transpose(scratch[...])[:8, :]
    a = across.astype(BF16)
    rest = across - a.astype(F32)
    b = rest.astype(BF16)
    c = (rest - b.astype(F32)).astype(BF16)
    total = jnp.zeros((8, 2 * splits), F32)
    outs = []
    for j in range(2):
        hot = jnp.where(
            iota((splits, 2 * splits), 1) == 2 * iota((splits, 2 * splits), 0) + j, 1.0, 0.0
        ).astype(BF16)
        outs.append(dot(a, hot) + (dot(b, hot) + dot(c, hot)))
    for l in range(levels):
        spread[l : l + 1, :] = outs[0][2 * l : 2 * l + 1, :] + outs[1][2 * l + 1 : 2 * l + 2, :]


def on_device(embeddings, root_centroids, member_ids, split_order, seed_rows):
    rows, width = embeddings.shape
    levels, splits = seed_rows.shape[:2]
    assert levels == 3
    comm = Comm(lax.axis_size(AXES), splits // 8)
    n, lead = comm.n, comm.lead
    own = splits // comm.blocks
    per = comm.blocks // lead
    scale = 0.5 / (float(width) ** 0.5)
    place = jnp.stack([comm.block, comm.me * rows, comm.me]).astype(jnp.int32)
    smem = pl.BlockSpec(memory_space=pltpu.SMEM)
    vmem = pl.BlockSpec(memory_space=pltpu.VMEM)
    geometry = dict(levels=levels, lead=lead, per=per, own=own)
    table = (splits, width)
    narrow = (splits, LANES)

    def struct(shape, dtype=F32):
        return jax.ShapeDtypeStruct(shape, dtype)

    def pieces_of(parts, extra=LANES):
        return [struct((per, own, parts * width + extra))] * lead

    def call(kernel, name, outs, scalars, args, scratch=(), limit=30, us=3):
        run = pl.pallas_call(
            kernel,
            name=name,
            out_shape=outs,
            in_specs=[smem] * len(scalars) + [vmem] * len(args),
            out_specs=[vmem] * len(outs),
            scratch_shapes=[pltpu.VMEM(s, F32) for s in scratch],
            compiler_params=pltpu.CompilerParams(vmem_limit_bytes=limit * 1024 * 1024),
            cost_estimate=pl.CostEstimate(
                flops=us * 200_000_000, bytes_accessed=0, transcendentals=0
            ),
        )
        return list(run(*scalars, *args))

    seeds = seed_rows.transpose(0, 2, 1)
    *sent, high, low, squares = call(
        functools.partial(pick_kernel, **geometry),
        "pick",
        pieces_of(levels) + [struct((rows, width), BF16)] * 2 + [struct((1, rows))],
        [place],
        [seeds, embeddings],
        [(splits, levels * width + LANES)],
    )
    sent_on = comm.scatter_send(sent, 0)
    cols, *roots = call(
        functools.partial(tables_kernel, levels=levels),
        "tables",
        [struct(narrow)] + [struct(table)] * levels,
        [place],
        [seeds, split_order, root_centroids],
    )
    sent_on, cols, roots = tie(sent_on, cols, roots)
    x = comm.spread_out(comm.add_up(sent, sent_on), 1)
    sent_on = comm.scatter_send(x, 1)
    early = call(
        functools.partial(means_kernel, **geometry),
        "means",
        pieces_of(2 * levels, 0) + [struct(table)] * (3 * (levels - 1)),
        [place],
        [seeds, split_order, member_ids, high, low],
        [(splits, 2 * levels * width)],
        us=8,
    )
    sent_on, early = tie(sent_on, early)
    early, rest = early[:lead], early[lead:]
    means, deltas, wholes = (rest[i * (levels - 1) :][: levels - 1] for i in range(3))
    delta_own = comm.scatter_rest(comm.add_up(x, sent_on), 2)
    x = delta_own[None]
    for step in range(len(comm.stages) - 1, 0, -1):
        got = comm.gather_send(x, step)
        if step == 1:
            early_x = comm.add_up(early, comm.scatter_send(early, 0))
            got, early_x = tie(got, early_x)
        x = jnp.concatenate([x] + got)
    pieces = [x] + comm.gather_send(x, 0)
    early_own = comm.scatter_rest(early_x, 1)
    proj, stat, small, shared, state, weight = call(
        functools.partial(project_kernel, scale=scale, **geometry),
        "project",
        [
            struct((splits, rows)),
            struct(narrow),
            struct(narrow),
            struct((8, splits)),
            struct((8, rows)),
            struct((1, rows)),
        ],
        [place],
        [*pieces, high, low, squares, roots[0], roots[1], cols, member_ids],
        [table, narrow],
    )
    projs, root_stats = [None, proj], [None, stat]
    for l in range(2, levels):
        made, root_stat = call(
            functools.partial(ahead_kernel, l=l, **geometry),
            f"ahead{l}",
            [struct((splits, rows)), struct(narrow)],
            [place],
            [*pieces, high, low, roots[l]],
            [table],
        )
        projs.append(made)
        root_stats.append(root_stat)
    weights_out = [weight]
    counts, start = [], roots[0]
    sums_own, smalls = [], []
    for l in range(levels):
        more = l + 1 < levels
        if l:
            outs = [
                struct(narrow),
                struct((8, rows)),
                struct((8, splits)),
                struct((1, rows)),
            ]
            small, state, count, weight, *shared = call(
                functools.partial(level_kernel, l=l, levels=levels, scale=scale),
                f"level{l}",
                outs + [struct((8, splits))] * more,
                [],
                [got, *projs[l : l + 2], stat, root_stats[l], small, state, cols, member_ids]
                + counts,
            )
            counts = [count]
            weights_out.append(weight)
            smalls.append(small)
            shared = shared[0] if more else None
        if more:
            got = comm.all_reduce(shared)
        args = [high, low, state, small]
        if more:
            args += [wholes[l], means[l], deltas[l], start]
        parts = 1 + more
        out = call(
            functools.partial(sums_kernel, l=l, **geometry),
            f"sums{l}",
            pieces_of(parts) + [struct(table)] * (l + 2 < levels),
            [place, split_order],
            args,
            [(splits, parts * width + LANES)] + [(2, splits, width)] * more,
        )
        if l + 2 < levels:
            start = out.pop()
        x = comm.add_up(out, comm.scatter_send(out, 0))
        if more:
            got, x = tie(got, x)
        sums_own.append(comm.scatter_rest(x, 1))
    (final,) = call(
        functools.partial(finish_kernel, levels=levels),
        "finish",
        [struct((2 * own, width + LANES))],
        [place],
        [*sums_own, *smalls, early_own, roots[0], delta_own],
    )
    x = final[None]
    for step in range(len(comm.stages) - 1, 0, -1):
        x = jnp.concatenate([x] + comm.gather_send(x, step))
    pieces = [x] + comm.gather_send(x, 0)
    centre, spread = call(
        functools.partial(place_kernel, **geometry),
        "place",
        [struct((2 * splits, width)), struct((levels, 2 * splits))],
        [place],
        pieces,
        [narrow],
    )
    return (centre, spread, jnp.concatenate(weights_out, axis=0))


def solution(mesh):
    in_specs = (P(AXES, None), P(), P(None, AXES), P(), P())
    out_specs = (P(), P(), P(None, AXES))
    return jax.shard_map(
        on_device, mesh=mesh, in_specs=in_specs, out_specs=out_specs, check_vma=False
    )
```
